32 devices in a mesh: grp: 2 (over x), tile: 4 (over z), mem: 4 (over y, core).
Axes of the slice: x: 2, y: 2, z: 4, core: 2. Of those that a mesh axis runs over, the one named last changes fastest.
Arguments:
- current_state: float32 [512, 2, 8192], P(('grp', 'mem'), None, 'tile'), may hold values from -6 to 6
- lagged_states: float32 [3, 4, 8, 512, 512], P(None, 'tile', ('grp', 'mem')), may hold values from -6 to 6
- water_depth: float32 [8192], P('tile'), may hold values from 0.4 to 1
- obs_cells: int32 [4096], replicated, may hold values from 0 to 8191, as said below
- obs_values: float32 [4096], replicated, may hold values from -6 to 6
- obs_errors: float32 [4096], replicated, may hold values from 0.5 to 2
- tile_obs: int32 [4, 8, 1024], P('tile', ('grp', 'mem')), may hold values from -1 to 4095, as said below
Outputs:
- analysis_state: float32 [512, 2, 8192], P(('grp', 'mem'), None, 'tile')
- smoothed_lags: float32 [3, 4, 8, 512, 512], P(None, 'tile', ('grp', 'mem'))
The draws below stay inside these ranges and needn't reach their ends.
Inputs may be any that keep to these rules, and one draw needn't show every extreme that they name: `obs_cells`: observation o lies in grid tile o // 1024, that is at a cell from (o // 1024) * 2048 to that plus 2048 - 1. `tile_obs`: each list holds distinct indices of observations in its own grid tile or the two beside it (periodically), used slots first and -1 after them; at least 256 slots are used in every list, all 1024 in some list.
All inputs are finite; a program needn't handle non-finite values. Where the reference program divides by a largest or mean magnitude, that divisor is 1e-20 or more.
Results may differ from the reference program's by a relative error of at most 0.0003.
Values sent between devices are 32-bit elements; how exact they have to be, the bound alone decides.
A program may use at most 64 MiB of HBM per device.

```python
import math
import jax
import jax.numpy as jnp
from jax import lax

TRIAL_TOTAL = 512
PATCH_POINTS = 256
OBS_DEV = 1024
ITERS = 6
LAGS = 3
MODEL_STEPS = 2
P_MAX = 1024
LOC = 512
PATCH_UNKNOWNS = 512
SUBT = 8
GRID = 4
CELLS_DEV = 2048
NCELLS = 8192
NOBS = 4096


def obs_layout(key):
    base = jax.random.fold_in(key, 11)
    key_cells, key_counts, key_full = jax.random.split(base, 3)
    offsets = jax.random.randint(key_cells, (GRID, OBS_DEV), 0, CELLS_DEV)
    obs_sites = (offsets + jnp.arange(GRID, dtype=jnp.int32)[:, None] * CELLS_DEV).reshape(NOBS)
    counts = jax.random.randint(key_counts, (GRID * SUBT,), P_MAX // 4, P_MAX + 1)
    full_tile = jax.random.randint(key_full, (), 0, GRID * SUBT)
    counts = jnp.where(jnp.arange(GRID * SUBT) == full_tile, P_MAX, counts)

    def one_tile(tile_number):
        grid_index = tile_number // SUBT
        part_index = tile_number % SUBT
        center = grid_index * CELLS_DEV + part_index * PATCH_POINTS + PATCH_POINTS // 2
        candidates = ((grid_index - 1) * OBS_DEV + jnp.arange(3 * OBS_DEV, dtype=jnp.int32)) % NOBS
        distance = jnp.abs(obs_sites[candidates] - center)
        distance = jnp.minimum(distance, NCELLS - distance)
        score = distance * (3 * OBS_DEV) + jnp.arange(3 * OBS_DEV, dtype=jnp.int32)
        chosen = candidates[jnp.argsort(score)[:P_MAX]]
        return jnp.where(jnp.arange(P_MAX) < counts[tile_number], chosen, -1)
    row_lists = jax.vmap(one_tile)(jnp.arange(GRID * SUBT, dtype=jnp.int32))
    return (obs_sites.astype(jnp.int32), row_lists.reshape(GRID, SUBT, P_MAX).astype(jnp.int32))


def draw_obs_cells(key, part):
    return obs_layout(key)[0]


def draw_tile_obs(key, part):
    return obs_layout(key)[1]


def levels(own_key, dims, pieces, low, top_value):
    def one(position, parts):
        heights = jax.random.uniform(jax.random.fold_in(jax.random.fold_in(own_key, 6), position), (parts,), jnp.float32, low / len(pieces), top_value / len(pieces))
        return jnp.repeat(jnp.exp(heights), dims[position] // parts).reshape((-1,) + (1,) * (len(dims) - position - 1))

    gain = one(*pieces[0])
    for cut in pieces[1:]:
        gain = gain * one(*cut)
    return gain


def scatter_about(own_key, shape, width, bound, pieces=(), kind=jnp.bfloat16):
    values = width * jax.random.normal(own_key, shape, jnp.float32)
    if pieces:
        values = values * levels(own_key, shape, pieces, -0.22, 0.18)
    return jnp.clip(values, -bound, bound).astype(kind)


def setup_inputs(seed: int = 0) -> dict:
    splits = jax.random.split(jax.random.key(seed), 8)
    return {
        "current_state": scatter_about(splits[0], (TRIAL_TOTAL, 2, NCELLS), 1.0, 6.0, ((0, 8), (2, 4)), jnp.float32),
        "lagged_states": scatter_about(splits[1], (LAGS, GRID, SUBT, TRIAL_TOTAL, PATCH_UNKNOWNS), 1.0, 6.0, ((1, 4), (2, 8)), jnp.float32),
        "water_depth": jnp.clip(jnp.exp(math.log(1.0) - 0.9162907 * jax.random.uniform(splits[2], (NCELLS,), jnp.float32) ** levels(splits[2], (NCELLS,), ((0, 4),), -0.2, 0.2)), 0.4, 1.0),
        "obs_cells": draw_obs_cells(jax.random.fold_in(splits[7], 71), 0),
        "obs_values": scatter_about(splits[4], (NOBS,), 1.0, 6.0, (), jnp.float32),
        "obs_errors": jnp.clip(jnp.exp(jax.random.uniform(splits[5], (NOBS,), jnp.float32, math.log(0.5), math.log(2.0))), 0.5, 2.0),
        "tile_obs": draw_tile_obs(jax.random.fold_in(splits[7], 71), 0),
    }


flux_scale = 0.9
wave_scale = 0.9
highest = lax.Precision.HIGHEST

def advance(free_elevation, fluid_speed, water_depth):
    for repeat in range(MODEL_STEPS):
        free_elevation = free_elevation - flux_scale * water_depth * (fluid_speed - jnp.roll(fluid_speed, 1, axis=-1))
        fluid_speed = fluid_speed - wave_scale * (jnp.roll(free_elevation, -1, axis=-1) - free_elevation)
    return (free_elevation, fluid_speed)

def inverse_root(matrix, members):
    row_bound = jnp.max(lax.optimization_barrier(jnp.sum(jnp.abs(matrix), axis=1)))
    identity = jnp.eye(members, dtype=jnp.float32)
    approx = matrix / row_bound
    root_inv = identity
    for repeat in range(ITERS):
        middle = 1.5 * identity - 0.5 * jnp.dot(root_inv, approx, precision=highest)
        approx = jnp.dot(approx, middle, precision=highest)
        root_inv = jnp.dot(middle, root_inv, precision=highest)
    return root_inv / jnp.sqrt(row_bound)

def analyse(states, predicted, obs_level, obs_spread, obs_sites, usable, center, cell_total):
    members = predicted.shape[0]
    mean_obs = lax.optimization_barrier(jnp.mean(predicted, axis=0))
    spread = predicted - mean_obs
    departure = obs_level - mean_obs
    distance = jnp.abs(obs_sites - center)
    distance = jnp.minimum(distance, cell_total - distance).astype(jnp.float32)
    weight = jnp.exp(-0.5 * (distance / LOC) ** 2) / (obs_spread * obs_spread)
    weight = jnp.where(usable, weight, jnp.zeros_like(weight))
    identity = jnp.eye(members, dtype=jnp.float32)
    precision_matrix = (members - 1) * identity + jnp.dot(spread * weight, spread.T, precision=highest)
    root_cover = inverse_root(precision_matrix, members)
    covariance = jnp.dot(root_cover, root_cover, precision=highest)
    mean_weight = jnp.dot(covariance, jnp.dot(spread, weight * departure, precision=highest), precision=highest)
    transform = math.sqrt(members - 1) * root_cover + mean_weight[:, None]
    state_mean = lax.optimization_barrier(jnp.mean(states, axis=1, keepdims=True))
    return state_mean + jnp.einsum('ij,liv->ljv', transform, states - state_mean, precision=highest)

def reference(current_state, lagged_states, water_depth, obs_cells, obs_values, obs_errors, tile_obs):
    free_elevation, fluid_speed = advance(current_state[:, 0], current_state[:, 1], water_depth)
    prior_fields = jnp.stack([free_elevation, fluid_speed], axis=1)
    predicted_all = free_elevation[:, obs_cells]

    def one_tile(tile_number):
        grid_index = tile_number // SUBT
        part_index = tile_number % SUBT
        initial_shift = (grid_index * CELLS_DEV + part_index * PATCH_POINTS).astype(jnp.int32)
        patch_field_slab = lax.dynamic_slice_in_dim(prior_fields, initial_shift, PATCH_POINTS, 2).reshape(TRIAL_TOTAL, PATCH_UNKNOWNS)
        lag_block = lagged_states[:, grid_index, part_index]
        row_list = tile_obs[grid_index, part_index]
        usable = row_list >= 0
        clamped = jnp.maximum(row_list, 0)
        predicted = jnp.take(predicted_all, clamped, axis=1)
        center = initial_shift + PATCH_POINTS // 2
        states = jnp.concatenate([patch_field_slab[None], lag_block], axis=0)
        return analyse(states, predicted, obs_values[clamped], obs_errors[clamped], obs_cells[clamped], usable, center, NCELLS)
    results = lax.map(one_tile, jnp.arange(GRID * SUBT, dtype=jnp.int32))
    results = results.reshape(GRID, SUBT, LAGS + 1, TRIAL_TOTAL, 2, PATCH_POINTS)
    analysis = results[:, :, 0].transpose(2, 3, 0, 1, 4).reshape(TRIAL_TOTAL, 2, NCELLS)
    older_out = results[:, :, 1:].reshape(GRID, SUBT, LAGS, TRIAL_TOTAL, PATCH_UNKNOWNS).transpose(2, 0, 1, 3, 4)
    return (analysis, older_out)
```

```python
import functools
import math

import jax
import jax.numpy as jnp
from jax import lax
from jax.experimental import pallas as pl
from jax.experimental.pallas import tpu as pltpu
from jax.sharding import PartitionSpec as P

OBS_DEV = 1024
ITERS = 6
MODEL_STEPS = 2
LOC = 512
EDGE = 128
UNROLL = 32

flux_scale = 0.9
wave_scale = 0.9
f32 = jnp.float32
bf16 = jnp.bfloat16

VMEM = pl.BlockSpec(memory_space=pltpu.VMEM)
SMEM = pl.BlockSpec(memory_space=pltpu.SMEM)


def params():
    return pltpu.CompilerParams(vmem_limit_bytes=56 * 1024 * 1024)


def cost(flops, moved):
    return pl.CostEstimate(flops=flops, bytes_accessed=moved, transcendentals=0)


def split(x):
    high = x.astype(bf16)
    return high, (x - high.astype(f32)).astype(bf16)


def dot(a, b):
    return jnp.dot(a, b, preferred_element_type=f32)


def product(a, b):
    return dot(a[0], b[0]) + (dot(a[0], b[1]) + dot(a[1], b[0]))


def shifted(array, axis, by):
    peers = lax.axis_size(axis)
    return lax.ppermute(array, axis, [(i, (i + by) % peers) for i in range(peers)])


def copy_rows(index_ref, table_ref, out_ref, count):
    def body(step, carry):
        base = pl.multiple_of(step * UNROLL, UNROLL)
        rows = [table_ref[pl.ds(index_ref[base + j], 1), :] for j in range(UNROLL)]
        for j in range(UNROLL):
            out_ref[pl.ds(base + j, 1), :] = rows[j]
        return carry

    lax.fori_loop(0, count // UNROLL, body, 0)


def paired(low, high):
    lane = lax.broadcasted_iota(jnp.int32, low.shape, low.ndim - 1)
    return jnp.where(lane < low.shape[-1] // 2, low, high)


def forecast_kernel(
    index_ref, state_ref, left_ref, right_ref, depth_ref, fields_ref, picked_ref, table, rows
):
    members, _, cells = state_ref.shape
    parts = fields_ref.shape[0]
    width = cells // parts
    total = cells + 2 * EDGE
    h = jnp.concatenate([left_ref[:, 0, :], state_ref[:, 0, :], right_ref[:, 0, :]], axis=1)
    u = jnp.concatenate([left_ref[:, 1, :], state_ref[:, 1, :], right_ref[:, 1, :]], axis=1)
    depth = flux_scale * depth_ref[...]
    for repeat in range(MODEL_STEPS):
        h = h - depth * (u - pltpu.roll(u, 1, 1))
        u = u - wave_scale * (pltpu.roll(h, total - 1, 1) - h)
    for part in range(parts):
        fields_ref[part, 0] = h[:, EDGE + part * width : EDGE + (part + 1) * width]
        fields_ref[part, 1] = u[:, EDGE + part * width : EDGE + (part + 1) * width]
    own = h[:, EDGE : EDGE + cells]
    table[...] = jnp.concatenate([own, own], axis=0).T
    count = rows.shape[0]
    copy_rows(index_ref, table, rows, count)
    picked_ref[...] = paired(rows[: count // 2, :], rows[count // 2 :, :])


def listed_kernel(index_ref, before_ref, here_ref, after_ref, out_ref, table, rows):
    half = here_ref.shape[0]
    for place, block_ref in enumerate((before_ref, here_ref, after_ref)):
        block = block_ref[...]
        turned = pltpu.roll(block, block.shape[1] // 2, 1)
        table[2 * place * half : (2 * place + 1) * half, :] = paired(block, turned)
        table[(2 * place + 1) * half : (2 * place + 2) * half, :] = paired(turned, block)
    parts, slots_half, _ = out_ref.shape
    count = 2 * slots_half
    copy_rows(index_ref, table, rows, parts * count)
    for part in range(parts):
        out_ref[part] = paired(
            rows[part * count : part * count + slots_half, :],
            rows[part * count + slots_half : (part + 1) * count, :],
        )


def facts_kernel(index_ref, facts_ref, out_ref, table):
    table[...] = facts_ref[...].T
    copy_rows(index_ref, table, out_ref, out_ref.shape[0])


def transform_kernel(
    cell_total, center_ref, arrived_ref, facts_ref, high_ref, low_ref, spread, near, root
):
    parts, half, lanes = arrived_ref.shape
    block = lanes // 2
    members = parts * block
    for part in range(parts):
        spread[:half, part * block : (part + 1) * block] = arrived_ref[part, :, :block]
        spread[half:, part * block : (part + 1) * block] = arrived_ref[part, :, block:]
    level = facts_ref[:, 0:1]
    sigma = facts_ref[:, 1:2]
    distance = jnp.abs(facts_ref[:, 2:3] - center_ref[0])
    distance = jnp.minimum(distance, float(cell_total) - distance)
    weight = jnp.exp(-0.5 * (distance / LOC) ** 2) / (sigma * sigma)
    weight = jnp.where(facts_ref[:, 3:4] > 0.0, weight, jnp.zeros_like(weight))
    predicted = spread[...]
    mean = jnp.sum(predicted, axis=1, keepdims=True) / members
    deviation = predicted - mean
    innovation = jnp.sum(deviation * (weight * (level - mean)), axis=0, keepdims=True)
    scaled = split((deviation * jnp.sqrt(weight)).T)
    across = (((1,), (1,)), ((), ()))
    gram = lax.dot_general(scaled[0], scaled[0], across, preferred_element_type=f32)
    mixed = lax.dot_general(scaled[0], scaled[1], across, preferred_element_type=f32)
    gram = gram + (mixed + mixed.T)
    row = lax.broadcasted_iota(jnp.int32, (members, members), 0)
    column = lax.broadcasted_iota(jnp.int32, (members, members), 1)

    def middle(value):
        return jnp.where(row == column, 1.5, 0.0) - 0.5 * value

    matrix = gram + jnp.where(row == column, float(members - 1), 0.0)
    bound = jnp.max(jnp.sum(jnp.abs(matrix), axis=0, keepdims=True))
    start = matrix / bound
    first = middle(start)
    root[...] = first
    near[...] = product(split(start), split(first))

    def newton_step(repeat, carry):
        y = split(near[...])
        z = split(root[...])
        t = split(middle(product(z, y)))
        near[...] = product(y, t)
        root[...] = product(t, z)
        return carry

    lax.fori_loop(0, ITERS - 2, newton_step, 0)
    z = split(root[...])
    t = split(middle(product(z, split(near[...]))))
    cover_root = product(t, z) / jnp.sqrt(bound)
    once = jnp.sum(cover_root * innovation, axis=1, keepdims=True)
    mean_weight = jnp.sum(cover_root * once, axis=0, keepdims=True)
    high, low = split(math.sqrt(members - 1) * cover_root + mean_weight)
    high_ref[...] = high
    low_ref[...] = low


def moved(states, high, low):
    mean = jnp.sum(states, axis=0, keepdims=True) / states.shape[0]
    return mean + product((high, low), split(states - mean))


def apply_fields_kernel(high_ref, low_ref, fields_ref, out_ref):
    parts, variables, block, width = fields_ref.shape
    for variable in range(variables):
        states = fields_ref[:, variable].reshape(parts * block, width)
        result = moved(states, high_ref[...], low_ref[...])
        out_ref[:, variable] = result.reshape(parts, block, width)


def apply_lags_kernel(high_ref, low_ref, lag_ref, out_ref):
    out_ref[0] = moved(lag_ref[0], high_ref[...], low_ref[...])


def per_device(
    current_state, lagged_states, water_depth, obs_cells, obs_values, obs_errors, tile_obs
):
    block = current_state.shape[0]
    cells = current_state.shape[2]
    parts = lax.axis_size("grp") * lax.axis_size("mem")
    tile_count = lax.axis_size("tile")
    tile_index = lax.axis_index("tile")
    part_index = lax.axis_index("grp") * lax.axis_size("mem") + lax.axis_index("mem")
    obs_total = obs_values.shape[0]
    width = cells // parts
    members = block * parts
    slots = tile_obs.shape[-1]
    group = ("grp", "mem")

    left = shifted(current_state[:, :, cells - EDGE :], "tile", 1)
    right = shifted(current_state[:, :, :EDGE], "tile", -1)
    depth_left = shifted(water_depth[cells - EDGE :], "tile", 1)
    depth_right = shifted(water_depth[:EDGE], "tile", -1)
    depth = jnp.concatenate([depth_left, water_depth, depth_right])[None]

    own_list = tile_obs[0, 0]
    relative = (jnp.maximum(own_list, 0) - (tile_index - 1) * OBS_DEV) % obs_total
    relative = jnp.where(own_list >= 0, relative, 0)
    relative = jnp.clip(relative, 0, 3 * OBS_DEV - 1)
    all_lists = lax.all_gather(relative, group, axis=0, tiled=True)
    local_cells = lax.dynamic_slice_in_dim(obs_cells, tile_index * OBS_DEV, OBS_DEV)
    local_cells = jnp.clip(local_cells - tile_index * cells, 0, cells - 1)

    def around(array):
        return jnp.concatenate(
            [
                lax.dynamic_slice_in_dim(
                    array, (tile_index + by) % tile_count * OBS_DEV, OBS_DEV
                )
                for by in (-1, 0, 1)
            ]
        )

    nothing = jnp.zeros((3 * OBS_DEV,), f32)
    facts_table = jnp.stack(
        [around(obs_values), around(obs_errors), around(obs_cells).astype(f32)] + [nothing] * 5
    )
    facts_rows = pl.pallas_call(
        facts_kernel,
        out_shape=jax.ShapeDtypeStruct((slots, 8), f32),
        in_specs=[SMEM, VMEM],
        out_specs=VMEM,
        scratch_shapes=[pltpu.VMEM((3 * OBS_DEV, 8), f32)],
        compiler_params=params(),
        cost_estimate=cost(0, 4 << 20),
        name="facts",
    )(relative, facts_table)
    usable = (own_list >= 0).astype(f32)
    facts = jnp.concatenate([facts_rows[:, :3], usable[:, None], facts_rows[:, 4:]], axis=1)

    fields, picked = pl.pallas_call(
        forecast_kernel,
        out_shape=(
            jax.ShapeDtypeStruct((parts, 2, block, width), f32),
            jax.ShapeDtypeStruct((OBS_DEV // 2, 2 * block), f32),
        ),
        in_specs=[SMEM] + [VMEM] * 4,
        out_specs=(VMEM, VMEM),
        scratch_shapes=[
            pltpu.VMEM((cells, 2 * block), f32),
            pltpu.VMEM((OBS_DEV, 2 * block), f32),
        ],
        compiler_params=params(),
        cost_estimate=cost(0, 8 << 20),
        name="forecast",
    )(local_cells, current_state, left, right, depth)

    before = shifted(picked, "tile", 1)
    after = shifted(picked, "tile", -1)
    regrouped = lax.all_to_all(fields, group, split_axis=0, concat_axis=0, tiled=True)

    listed = pl.pallas_call(
        listed_kernel,
        out_shape=jax.ShapeDtypeStruct((parts, slots // 2, 2 * block), f32),
        in_specs=[SMEM] + [VMEM] * 3,
        out_specs=VMEM,
        scratch_shapes=[
            pltpu.VMEM((3 * OBS_DEV, 2 * block), f32),
            pltpu.VMEM((parts * slots, 2 * block), f32),
        ],
        compiler_params=params(),
        cost_estimate=cost(0, 24 << 20),
        name="listed",
    )(all_lists, before, picked, after)
    arrived = lax.all_to_all(listed, group, split_axis=0, concat_axis=0, tiled=True)

    center = tile_index * cells + part_index * width + width // 2
    high, low = pl.pallas_call(
        functools.partial(transform_kernel, cells * tile_count),
        out_shape=(jax.ShapeDtypeStruct((members, members), bf16),) * 2,
        in_specs=[SMEM, VMEM, VMEM],
        out_specs=(VMEM, VMEM),
        scratch_shapes=[
            pltpu.VMEM((slots, members), f32),
            pltpu.VMEM((members, members), f32),
            pltpu.VMEM((members, members), f32),
        ],
        compiler_params=params(),
        cost_estimate=cost(2 * 51 * members**3, 8 << 20),
        name="transform",
    )(center.astype(f32)[None], arrived, facts)

    analysed = pl.pallas_call(
        apply_fields_kernel,
        out_shape=jax.ShapeDtypeStruct(fields.shape, f32),
        in_specs=[VMEM] * 3,
        out_specs=VMEM,
        compiler_params=params(),
        cost_estimate=cost(2 * 3 * members**3, 4 << 20),
        name="apply_fields",
    )(high, low, regrouped)
    returned = lax.all_to_all(analysed, group, split_axis=0, concat_axis=0, tiled=True)

    lags = lagged_states.shape[0]
    unknowns = lagged_states.shape[-1]
    whole = pl.BlockSpec((members, members), lambda i: (0, 0))
    one = pl.BlockSpec((1, members, unknowns), lambda i: (i, 0, 0))
    older = pl.pallas_call(
        apply_lags_kernel,
        grid=(lags,),
        out_shape=jax.ShapeDtypeStruct((lags, members, unknowns), f32),
        in_specs=[whole, whole, one],
        out_specs=one,
        compiler_params=params(),
        cost_estimate=cost(2 * 9 * members**3, 16 << 20),
        name="apply_lags",
    )(high, low, lagged_states[:, 0, 0])
    analysis_state = returned.transpose(2, 1, 0, 3).reshape(block, 2, cells)
    return (analysis_state, older[:, None, None])


def solution(mesh):
    placed = (
        P(("grp", "mem"), None, "tile"),
        P(None, "tile", ("grp", "mem"), None, None),
        P("tile"),
        P(),
        P(),
        P(),
        P("tile", ("grp", "mem"), None),
    )
    return jax.shard_map(
        per_device,
        mesh=mesh,
        in_specs=placed,
        out_specs=(P(("grp", "mem"), None, "tile"), P(None, "tile", ("grp", "mem"), None, None)),
        check_vma=False,
    )
```
